32 devices in a mesh: slab: 8 (over y, x, core), col: 4 (over z).
Axes of the slice: x: 2, y: 2, z: 4, core: 2. Of those that a mesh axis runs over, the one named last changes fastest.
Arguments:
- hamiltonian_blocks: bfloat16 [128, 9, 128, 128], P('slab'), may hold values from -0.0625 to 0.0625
- block_columns: int32 [128, 9], P('slab'), may hold values from 0 to 127, as said below
- probe: bfloat16 [16384, 2048], P('slab', 'col'), may hold values from -6 to 6
- previous: float32 [16384, 2048], P('slab', 'col'), may hold values from -6 to 6
- current: float32 [16384, 2048], P('slab', 'col'), may hold values from -6 to 6
- orbital_weight: float32 [16384], P('slab'), may hold values from 0.1 to 10
Outputs:
- last_previous: float32 [16384, 2048], P('slab', 'col')
- last_current: float32 [16384, 2048], P('slab', 'col')
- moments: float32 [3, 2048], P(None, 'col')
The draws below stay inside these ranges and needn't reach their ends.
Inputs may be any that keep to these rules, and one draw needn't show every extreme that they name: `block_columns`: the 9 entries of a row are distinct block columns within 5 of the row's own block row, counted cyclically modulo 128; they include the row itself and the block rows 5 before and 5 after it.
All inputs are finite; a program needn't handle non-finite values.
Results may differ from the reference program's by a relative error of at most 0.0024.
Values may be sent and summed in bfloat16 or wider, within the bound.
A program may use at most 192 MiB of HBM per device.

```python
import math
import jax
import jax.numpy as jnp
from jax import lax

BLK = 128
BAND = 5
NB = 9
TERMS = 3
NBR = 128
NORB = 16384
COLS = 2048


def draw_block_columns(key, part):
    count = 2 * BAND - 2
    scores = jax.random.randint(key, (NBR, count), 0, 1 << 20) * count + jnp.arange(count)[None, :]
    picked = jnp.argsort(scores, axis=1)[:, :NB - 3]
    offsets = jnp.where(picked < BAND - 1, picked - (BAND - 1), picked - BAND + 2)
    fixed_part = jnp.broadcast_to(jnp.array([0, -BAND, BAND], jnp.int32)[None, :], (NBR, 3))
    every = jnp.concatenate([fixed_part, offsets.astype(jnp.int32)], axis=1)
    rowid = jnp.arange(NBR, dtype=jnp.int32)[:, None]
    return ((rowid + every) % NBR).astype(jnp.int32)


def steps_of(own_key, extent, shards, low, largest):
    gain = 1.0
    for dim, shards_of in shards:
        draws = jax.random.uniform(jax.random.fold_in(jax.random.fold_in(own_key, 6), dim), (shards_of,), jnp.float32, low / len(shards), largest / len(shards))
        gain = gain * jnp.repeat(jnp.exp(draws), extent[dim] // shards_of).reshape((-1,) + (1,) * (len(extent) - 1 - dim))
    return gain


def centred(own_key, shape, deviation, most, pieces=(), kind=jnp.bfloat16):
    values = deviation * jax.random.normal(own_key, shape, jnp.float32)
    if pieces:
        values = values * steps_of(own_key, shape, pieces, -0.22, 0.18)
    return jnp.clip(values, -most, most).astype(kind)


def setup_inputs(seed: int = 0) -> dict:
    arg_keys = jax.random.split(jax.random.key(seed), 7)
    return {
        "hamiltonian_blocks": centred(arg_keys[0], (NBR, NB, BLK, BLK), (8 * NB * BLK) ** -0.5, 0.0625, ((0, 8),)),
        "block_columns": draw_block_columns(jax.random.fold_in(arg_keys[6], 71), 0),
        "probe": centred(arg_keys[2], (NORB, COLS), 1.0, 6.0, ((0, 8), (1, 4))),
        "previous": centred(arg_keys[3], (NORB, COLS), 1.0, 6.0, ((0, 8), (1, 4)), jnp.float32),
        "current": centred(arg_keys[4], (NORB, COLS), 1.0, 6.0, ((0, 8), (1, 4)), jnp.float32),
        "orbital_weight": jnp.clip(jnp.exp(math.log(10.0) - 4.6051702 * jax.random.uniform(arg_keys[5], (NORB,), jnp.float32) ** steps_of(arg_keys[5], (NORB,), ((0, 8),), -0.2, 0.2)), 0.1, 10.0),
    }


def reference(hamiltonian_blocks, block_columns, probe, previous, current, orbital_weight):
    total = hamiltonian_blocks.shape[0] * BLK
    weights = orbital_weight[:, None] * probe.astype(jnp.float32) / total
    results = []
    for term in range(TERMS):
        source = current.astype(jnp.bfloat16).reshape(NBR, BLK, -1)

        def one_row(pair):
            blocks, columns = pair
            picked = source[columns]
            return jnp.einsum("sij,sjc->ic", blocks.astype(jnp.float32), picked.astype(jnp.float32))

        product = lax.map(one_row, (hamiltonian_blocks, block_columns)).reshape(total, -1)
        upcoming = 2.0 * product - previous
        results.append(jnp.sum(weights * upcoming, axis=0))
        previous, current = current, upcoming
    return previous, current, jnp.stack(results)
```

```python
import functools

import jax
import jax.numpy as jnp
from jax import lax
from jax.experimental import pallas as pl
from jax.experimental.pallas import tpu as pltpu
from jax.sharding import PartitionSpec as P

BAND = 5
TERMS = 3
LANES = 128
CHUNK = 256
GROUP = 2


def kernel(
    n, col_hbm, ow_hbm, h_hbm, probe_hbm, prev_hbm, cur_hbm,
    tb, mom,
    col_ref, ow_ref, hv, hb, ext, wts, pv,
    in_sem, send_sem, recv_sem, msend, mrecv, known,
):
    me = lax.axis_index("slab")
    rows, slots, w, _ = hv.shape
    chunks, height, cc = wts.shape
    total = n * rows
    rim = BAND * w
    gw = GROUP * w
    pairs = rows // GROUP
    edge = -(-BAND // GROUP)
    depth = gw + 2 * rim
    first = me * rows
    far = lax.rem(me, 2)
    near = 1 - far

    def columns(c):
        return pl.ds(c * cc, cc)

    inside = BAND - GROUP
    parts = ((0, inside), (inside, BAND))

    def layers(side, a, b):
        return (1 - side) * a * w + side * (BAND - b) * w

    def pieces(c, side):
        return ((0, 1), (1, inside), (inside, BAND)) if c == 0 and side is far else ((0, BAND),)

    def rim_in(c, side, k):
        a, b = pieces(c, side)[k]
        start = pl.multiple_of(side * (height - rim) + layers(side, a, b), w)
        return pltpu.make_async_copy(
            cur_hbm.at[pl.ds(start, (b - a) * w), columns(c)],
            tb.at[1, c, pl.ds(start, (b - a) * w)],
            in_sem.at[3 * c + side] if k == 0 else in_sem.at[3 * chunks + 3 + chunks + k],
        )

    inner = height - 2 * rim
    inner_in = [
        pltpu.make_async_copy(
            cur_hbm.at[pl.ds(rim, inner), columns(c)], tb.at[1, c, pl.ds(rim, inner)],
            in_sem.at[3 * c + 2])
        for c in range(chunks)
    ]
    base = 3 * chunks
    h_in = pltpu.make_async_copy(h_hbm, hv, in_sem.at[base])
    probe_in = pltpu.make_async_copy(probe_hbm, pv, in_sem.at[base + 1])
    col_in = pltpu.make_async_copy(col_hbm, col_ref, in_sem.at[base + 2])
    ow_in = pltpu.make_async_copy(ow_hbm, ow_ref, in_sem.at[base + 3])
    prev_in = [
        pltpu.make_async_copy(prev_hbm.at[:, columns(c)], tb.at[0, c], in_sem.at[base + 4 + c])
        for c in range(chunks)
    ]
    barrier = pltpu.get_barrier_semaphore()

    def greet(semaphore, distance):
        for other in (n - distance, distance):
            pl.semaphore_signal(
                semaphore, inc=1, device_id={"slab": lax.rem(me + other, n)},
                device_id_type=pl.DeviceIdType.MESH,
            )

    greet(barrier, 1)
    for c in range(chunks):
        for side in (far, near):
            for k in range(len(pieces(c, side))):
                rim_in(c, side, k).start()

    def halo(t, c, side, part, a=None, b=None):
        if a is None:
            a, b = parts[part]
        size = (b - a) * w
        offset = layers(side, a, b)
        source = pl.multiple_of(rim + side * (height - rim) + offset, w)
        target = pl.multiple_of((1 - side) * (rim + height) + offset, w)
        return pltpu.make_async_remote_copy(
            src_ref=ext.at[t, c, pl.ds(source, size)],
            dst_ref=ext.at[t, c, pl.ds(target, size)],
            send_sem=send_sem, recv_sem=recv_sem.at[t, c, 1 - side, part],
            device_id={"slab": lax.rem(me + n - 1 + 2 * side, n)},
            device_id_type=pl.DeviceIdType.MESH,
        )

    def cast(c, start, steps):
        def body(i, carry):
            at = pl.multiple_of(start + i * w, w)
            ext[0, c, pl.ds(pl.multiple_of(rim + at, w), w)] = tb[1, c, pl.ds(at, w)].astype(jnp.bfloat16)
            return carry

        lax.fori_loop(0, steps, body, 0)

    rounds = known.shape[0]
    for c in range(chunks):
        for side in (far, near):
            for k, (a, b) in enumerate(pieces(c, side)):
                rim_in(c, side, k).wait()
                cast(c, side * (height - rim) + layers(side, a, b), b - a)
                if c == 0 and side is far and k == 0:
                    pl.semaphore_wait(barrier, 2)
                for part, (low, high) in enumerate(parts):
                    low, high = max(low, a), min(high, b)
                    if low < high:
                        halo(0, c, side, part, low, high).start()
            if c == 0 and side is far:
                for copy in inner_in:
                    copy.start()
                col_in.start()
                h_in.start()
                ow_in.start()
                probe_in.start()
                for copy in prev_in:
                    copy.start()
                greet(known.at[0], 1)
    for c in range(chunks):
        inner_in[c].wait()
        cast(c, rim, inner // w)

    col_in.wait()
    h_in.wait()
    zero = jnp.zeros((w, w), jnp.bfloat16)

    def build(p, carry):
        for half in range(GROUP):
            r = p * GROUP + half
            places = []
            for s in range(slots):
                x = col_ref[r, s] - (first + r) + BAND
                x = jnp.where(x < 0, x + total, x)
                places.append(jnp.where(x >= total, x - total, x))
            for d in range(GROUP + 2 * BAND):
                place = d - half
                if place < 0 or place > 2 * BAND:
                    block = zero
                else:
                    slot = jnp.int32(0)
                    hit = jnp.int32(0)
                    for s in range(slots):
                        same = places[s] == place
                        slot = jnp.where(same, s, slot)
                        hit = jnp.where(same, 1, hit)
                    block = jnp.where(hit == 1, hv[r, slot], zero)
                hb[p, half * w:(half + 1) * w, d * w:(d + 1) * w] = block
        return carry

    lax.fori_loop(0, pairs, build, 0)

    probe_in.wait()
    ow_in.wait()
    eye = lax.broadcasted_iota(jnp.int32, (w, w), 0) == lax.broadcasted_iota(jnp.int32, (w, w), 1)

    def weigh(r, carry):
        row = jnp.broadcast_to(ow_ref[pl.ds(r, 1), :], (w, w))
        column = jnp.sum(jnp.where(eye, row, 0.0), axis=1, keepdims=True) / (total * w)
        at = pl.multiple_of(r * w, w)
        for c in range(chunks):
            wts[c, pl.ds(at, w)] = column * pv[pl.ds(at, w), c * cc:(c + 1) * cc].astype(jnp.float32)
        return carry

    lax.fori_loop(0, rows, weigh, 0)
    for copy in prev_in:
        copy.wait()

    def tile(t, c, p, acc):
        at = pl.multiple_of(p * gw, gw)
        product = jnp.dot(hb[p], ext[t, c, pl.ds(at, depth)], preferred_element_type=jnp.float32)
        upcoming = 2.0 * product - tb[t % 2, c, pl.ds(at, gw)]
        tb[t % 2, c, pl.ds(at, gw)] = upcoming
        if t + 1 < TERMS:
            ext[t + 1, c, pl.ds(pl.multiple_of(rim + at, w), gw)] = upcoming.astype(jnp.bfloat16)
        y = wts[c, pl.ds(at, gw)] * upcoming
        return acc + jnp.sum(y.reshape(gw // 8, 8, cc), axis=0)

    def moments(t, k, rest=None):
        block = mom.at[t, me] if rest is None else rest
        return pltpu.make_async_remote_copy(
            src_ref=block, dst_ref=block, send_sem=msend, recv_sem=mrecv.at[t],
            device_id={"slab": lax.rem(me + k, n)}, device_id_type=pl.DeviceIdType.MESH,
        )

    def spread(start, stop):
        for k in range(start, stop):
            pl.semaphore_wait(known.at[k], 2)
            if k + 1 < rounds:
                greet(known.at[k + 1], 2 ** (k + 1))

    for t in range(TERMS):
        for c in range(chunks):
            acc = jnp.zeros((8, cc), jnp.float32)
            acc = lax.fori_loop(edge, pairs - edge, lambda p, a: tile(t, c, p, a), acc)
            for side in (near, far):
                def rim_tile(i, a):
                    return tile(t, c, (1 - side) * (edge - 1 - i) + side * (pairs - edge + i), a)

                halo(t, c, 1 - side, 0).wait_recv()
                acc = lax.fori_loop(0, edge - 1, rim_tile, acc)
                halo(t, c, 1 - side, 1).wait_recv()
                acc = rim_tile(edge - 1, acc)
                if t + 1 < TERMS:
                    for part in range(2):
                        halo(t + 1, c, side, part).start()
            total_row = jnp.sum(acc, axis=0, keepdims=True)
            for k in range(cc // LANES):
                mom[t, me, pl.ds(c * (cc // LANES) + k, 1), :] = total_row[:, k * LANES:(k + 1) * LANES]
            if t == 0:
                spread(0 if c == 0 else 1, 1 if c + 1 < chunks else rounds)
        for k in range(1, n):
            moments(t, k).start()

    pltpu.make_async_remote_copy(
        src_ref=ext.at[:, :, pl.ds(0, 2 * rim)], dst_ref=ext.at[:, :, pl.ds(0, 2 * rim)],
        send_sem=send_sem, recv_sem=msend, device_id={"slab": lax.rem(me + 1, n)},
        device_id_type=pl.DeviceIdType.MESH,
    ).wait_send()
    others = mom.at[:, pl.ds(0, n - 1)]
    moments(0, 1, others).wait_send()
    for t in range(TERMS):
        moments(t, 1, mom.at[t, pl.ds(0, n - 1)]).wait_recv()


def finish(tb, mom, last_prev, last_cur, mom_hbm, row_sums, sem):
    terms, n, lanes_of, _ = mom.shape
    _, chunks, _, cc = tb.shape
    copies = []
    for c in range(chunks):
        for k, out in enumerate((last_cur, last_prev)):
            source = (terms - 1 + k) % 2
            copies.append(pltpu.make_async_copy(
                tb.at[source, c], out.at[:, pl.ds(c * cc, cc)], sem.at[2 * c + k]))
    for copy in copies:
        copy.start()
    for t in range(terms):
        whole = mom[t, 0]
        for i in range(1, n):
            whole = whole + mom[t, i]
        for k in range(lanes_of):
            row_sums[t:t + 1, k * LANES:(k + 1) * LANES] = whole[k:k + 1, :]
    copies.append(pltpu.make_async_copy(row_sums, mom_hbm, sem.at[2 * chunks]))
    copies[-1].start()
    for copy in copies:
        copy.wait()


def local(hamiltonian_blocks, block_columns, probe, previous, current, orbital_weight):
    n = lax.axis_size("slab")
    rows, slots, w, _ = hamiltonian_blocks.shape
    height, cols = current.shape
    cc = min(CHUNK, cols)
    chunks = cols // cc
    vmem = pl.BlockSpec(memory_space=pltpu.VMEM)
    hbm = pl.BlockSpec(memory_space=pltpu.HBM)
    bf16, f32 = jnp.bfloat16, jnp.float32
    grant = 67043328 - 4 * (2 * height * cols + TERMS * n * cols) - (64 << 10)
    tb, mom = pl.pallas_call(
        functools.partial(kernel, n),
        out_shape=(
            pltpu.VMEM((2, chunks, height, cc), f32),
            pltpu.VMEM((TERMS, n, cols // LANES, LANES), f32),
        ),
        in_specs=[hbm] * 6,
        out_specs=(vmem, vmem),
        scratch_shapes=[
            pltpu.SMEM((rows, slots), jnp.int32),
            pltpu.VMEM((rows, w), f32),
            pltpu.VMEM((rows, slots, w, w), bf16),
            pltpu.VMEM((rows // GROUP, GROUP * w, (GROUP + 2 * BAND) * w), bf16),
            pltpu.VMEM((TERMS, chunks, height + 2 * BAND * w, cc), bf16),
            pltpu.VMEM((chunks, height, cc), f32),
            pltpu.VMEM((height, cols), bf16),
            pltpu.SemaphoreType.DMA((4 * chunks + 6,)),
            pltpu.SemaphoreType.DMA,
            pltpu.SemaphoreType.DMA((TERMS, chunks, 2, 2)),
            pltpu.SemaphoreType.DMA,
            pltpu.SemaphoreType.DMA((TERMS,)),
            pltpu.SemaphoreType.REGULAR((max(1, (n // 2 - 1).bit_length()),)),
        ],
        compiler_params=pltpu.CompilerParams(
            collective_id=0, has_side_effects=True, vmem_limit_bytes=grant,
        ),
    )(block_columns, orbital_weight.reshape(rows, w), hamiltonian_blocks, probe, previous, current)
    return pl.pallas_call(
        finish,
        out_shape=(
            jax.ShapeDtypeStruct((height, cols), f32),
            jax.ShapeDtypeStruct((height, cols), f32),
            jax.ShapeDtypeStruct((TERMS, cols), f32),
        ),
        in_specs=[vmem, vmem],
        out_specs=(hbm, hbm, hbm),
        scratch_shapes=[
            pltpu.VMEM((TERMS, cols), f32),
            pltpu.SemaphoreType.DMA((2 * chunks + 1,)),
        ],
        compiler_params=pltpu.CompilerParams(vmem_limit_bytes=16 * 1024 * 1024),
    )(tb, mom)


def solution(mesh):
    return jax.shard_map(
        local,
        mesh=mesh,
        in_specs=(
            P("slab", None, None, None),
            P("slab", None),
            P("slab", "col"),
            P("slab", "col"),
            P("slab", "col"),
            P("slab"),
        ),
        out_specs=(P("slab", "col"), P("slab", "col"), P(None, "col")),
        check_vma=False,
    )
```

```python
import functools

import jax
import jax.numpy as jnp
from jax import lax
from jax.experimental import pallas as pl
from jax.experimental.pallas import tpu as pltpu
from jax.sharding import PartitionSpec as P

BAND = 5
TERMS = 3
LANES = 128
CHUNK = 256
GROUP = 2
LEAD = 3


def kernel(
    n, col_hbm, ow_hbm, h_hbm, probe_hbm, prev_hbm, cur_hbm,
    tb, mom,
    col_ref, ow_ref, hv, hb, ext, wts, pv,
    in_sem, send_sem, recv_sem, msend, mrecv, known, gate_sem, turn,
):
    me = lax.axis_index("slab")
    rows, slots, w, _ = hv.shape
    chunks, height, cc = wts.shape
    total = n * rows
    rim = BAND * w
    gw = GROUP * w
    pairs = rows // GROUP
    edge = -(-BAND // GROUP)
    depth = gw + 2 * rim
    first = me * rows
    far = lax.rem(me, 2)
    near = 1 - far

    def columns(c):
        return pl.ds(c * cc, cc)

    inside = BAND - GROUP
    parts = ((0, inside), (inside, BAND))

    def layers(side, a, b):
        return (1 - side) * a * w + side * (BAND - b) * w

    def pieces(c, side):
        return ((0, 1), (1, inside), (inside, BAND)) if c == 0 and side is far else ((0, BAND),)

    def rim_in(c, side, k):
        a, b = pieces(c, side)[k]
        start = pl.multiple_of(side * (height - rim) + layers(side, a, b), w)
        return pltpu.make_async_copy(
            cur_hbm.at[pl.ds(start, (b - a) * w), columns(c)],
            tb.at[1, c, pl.ds(start, (b - a) * w)],
            in_sem.at[6 + (k if c == 0 and side is far else 2 * c + (2 if side is far else 3))],
        )

    inner = height - 2 * rim
    inner_in = [
        pltpu.make_async_copy(
            cur_hbm.at[pl.ds(rim, inner), columns(c)], tb.at[1, c, pl.ds(rim, inner)],
            in_sem.at[0])
        for c in range(chunks)
    ]
    h_in = pltpu.make_async_copy(h_hbm, hv, in_sem.at[1])
    probe_in = pltpu.make_async_copy(probe_hbm, pv, in_sem.at[2])
    col_in = pltpu.make_async_copy(col_hbm, col_ref, in_sem.at[3])
    ow_in = pltpu.make_async_copy(ow_hbm, ow_ref, in_sem.at[4])
    prev_in = [
        pltpu.make_async_copy(prev_hbm.at[:, columns(c)], tb.at[0, c], in_sem.at[5])
        for c in range(chunks)
    ]
    barrier = pltpu.get_barrier_semaphore()

    def greet(semaphore, distance):
        for other in (n - distance, distance):
            pl.semaphore_signal(
                semaphore, inc=1, device_id={"slab": lax.rem(me + other, n)},
                device_id_type=pl.DeviceIdType.MESH,
            )

    greet(barrier, 1)
    for c in range(chunks):
        for side in (far, near):
            for k in range(len(pieces(c, side))):
                rim_in(c, side, k).start()

    def hops(chip):
        return lax.rem(chip, 2) + lax.rem(chip // 2, 2)

    chip = me // 2
    every = n // 2
    mine = hops(lax.rem(chip + every - 1 + 2 * far, every))
    other = hops(lax.rem(chip + every - 1 + 2 * near, every))
    last = (TERMS - 1, chunks - 1)

    def halo(t, c, side, part, a=None, b=None, gate=None):
        if a is None:
            a, b = parts[part]
        size = (b - a) * w
        offset = layers(side, a, b)
        source = pl.multiple_of(rim + side * (height - rim) + offset, w)
        target = pl.multiple_of((1 - side) * (rim + height) + offset, w)
        return pltpu.make_async_remote_copy(
            src_ref=ext.at[t, c, pl.ds(source, size)],
            dst_ref=ext.at[t, c, pl.ds(target, size)],
            send_sem=send_sem if gate is None else gate,
            recv_sem=recv_sem.at[t % 2, c, 1 - side, part],
            device_id={"slab": lax.rem(me + n - 1 + 2 * side, n)},
            device_id_type=pl.DeviceIdType.MESH,
        )

    def cast(c, start, steps):
        def body(i, carry):
            at = pl.multiple_of(start + i * w, w)
            ext[0, c, pl.ds(pl.multiple_of(rim + at, w), w)] = tb[1, c, pl.ds(at, w)].astype(jnp.bfloat16)
            return carry

        lax.fori_loop(0, steps, body, 0)

    rounds = known.shape[0]
    for c in range(chunks):
        for side in (far, near):
            for k, (a, b) in enumerate(pieces(c, side)):
                rim_in(c, side, k).wait()
                cast(c, side * (height - rim) + layers(side, a, b), b - a)
                if c == 0 and side is far and k == 0:
                    pl.semaphore_wait(barrier, 2)
                for part, (low, high) in enumerate(parts):
                    low, high = max(low, a), min(high, b)
                    if low < high:
                        halo(0, c, side, part, low, high).start()
            if c == 0 and side is far:
                for copy in inner_in:
                    copy.start()
                col_in.start()
                h_in.start()
                ow_in.start()
                probe_in.start()
                for copy in prev_in:
                    copy.start()
                greet(known.at[0], 1)
    inside_of = tb.at[1, :, pl.ds(rim, inner)]
    pltpu.make_async_copy(inside_of, inside_of, in_sem.at[0]).wait()
    for c in range(chunks):
        cast(c, rim, inner // w)

    col_in.wait()
    h_in.wait()
    zero = jnp.zeros((w, w), jnp.bfloat16)

    def build(p, carry):
        for half in range(GROUP):
            r = p * GROUP + half
            places = []
            for s in range(slots):
                x = col_ref[r, s] - (first + r) + BAND
                x = jnp.where(x < 0, x + total, x)
                places.append(jnp.where(x >= total, x - total, x))
            for d in range(GROUP + 2 * BAND):
                place = d - half
                if place < 0 or place > 2 * BAND:
                    block = zero
                else:
                    slot = jnp.int32(0)
                    hit = jnp.int32(0)
                    for s in range(slots):
                        same = places[s] == place
                        slot = jnp.where(same, s, slot)
                        hit = jnp.where(same, 1, hit)
                    block = jnp.where(hit == 1, hv[r, slot], zero)
                hb[p, half * w:(half + 1) * w, d * w:(d + 1) * w] = block
        return carry

    lax.fori_loop(0, pairs, build, 0)

    probe_in.wait()
    ow_in.wait()
    eye = lax.broadcasted_iota(jnp.int32, (w, w), 0) == lax.broadcasted_iota(jnp.int32, (w, w), 1)

    def weigh(r, carry):
        row = jnp.broadcast_to(ow_ref[pl.ds(r, 1), :], (w, w))
        column = jnp.sum(jnp.where(eye, row, 0.0), axis=1, keepdims=True) / (total * w)
        at = pl.multiple_of(r * w, w)
        for c in range(chunks):
            wts[c, pl.ds(at, w)] = column * pv[pl.ds(at, w), c * cc:(c + 1) * cc].astype(jnp.float32)
        return carry

    lax.fori_loop(0, rows, weigh, 0)
    pltpu.make_async_copy(tb.at[0], tb.at[0], in_sem.at[5]).wait()

    def tile(t, c, p, acc):
        at = pl.multiple_of(p * gw, gw)
        product = jnp.dot(hb[p], ext[t, c, pl.ds(at, depth)], preferred_element_type=jnp.float32)
        upcoming = 2.0 * product - tb[t % 2, c, pl.ds(at, gw)]
        tb[t % 2, c, pl.ds(at, gw)] = upcoming
        if t + 1 < TERMS:
            ext[t + 1, c, pl.ds(pl.multiple_of(rim + at, w), gw)] = upcoming.astype(jnp.bfloat16)
        y = wts[c, pl.ds(at, gw)] * upcoming
        return acc + jnp.sum(y.reshape(gw // 8, 8, cc), axis=0)

    def moments(final, k, first=me, count=1):
        terms = pl.ds(TERMS - 1, 1) if final else pl.ds(0, TERMS - 1)
        block = mom.at[pl.ds(first, count), terms]
        return pltpu.make_async_remote_copy(
            src_ref=block, dst_ref=block, send_sem=msend, recv_sem=mrecv.at[final],
            device_id={"slab": lax.rem(me + k, n)}, device_id_type=pl.DeviceIdType.MESH,
        )

    def spread(start, stop):
        for k in range(start, stop):
            pl.semaphore_wait(known.at[k], 2)
            if k + 1 < rounds:
                greet(known.at[k + 1], 2 ** (k + 1))

    for t in range(TERMS):
        for c in range(chunks):
            acc = jnp.zeros((8, cc), jnp.float32)
            acc = lax.fori_loop(edge, pairs - edge, lambda p, a: tile(t, c, p, a), acc)
            for side in (near, far):
                def rim_tile(i, a):
                    return tile(t, c, (1 - side) * (edge - 1 - i) + side * (pairs - edge + i), a)

                if (t, c) == last and side is far:
                    halo(t, c, side, 0, 0, LEAD, gate_sem).wait_send()

                    @pl.when(mine > other)
                    def _():
                        pl.semaphore_signal(
                            turn, inc=1, device_id={"slab": lax.rem(me + n - 1 + 2 * near, n)},
                            device_id_type=pl.DeviceIdType.MESH)

                    @pl.when(mine < other)
                    def _():
                        pl.semaphore_wait(turn, 1)
                        halo(t, c, side, 1).start()

                halo(t, c, 1 - side, 0).wait_recv()
                acc = lax.fori_loop(0, edge - 1, rim_tile, acc)
                halo(t, c, 1 - side, 1).wait_recv()
                if (t, c) == last and side is far:
                    for k in range(1, n):
                        moments(0, k).start()
                acc = rim_tile(edge - 1, acc)
                if t + 1 < TERMS:
                    if (t + 1, c) == last and side is far:
                        halo(t + 1, c, side, 0, 0, LEAD, gate_sem).start()
                        if LEAD < inside:
                            halo(t + 1, c, side, 0, LEAD, inside).start()
                        pl.when(mine >= other)(halo(t + 1, c, side, 1).start)
                    else:
                        for part in range(2):
                            halo(t + 1, c, side, part).start()
            total_row = jnp.sum(acc, axis=0, keepdims=True)
            for k in range(cc // LANES):
                mom[me, t, pl.ds(c * (cc // LANES) + k, 1), :] = total_row[:, k * LANES:(k + 1) * LANES]
            if t == 0:
                spread(0 if c == 0 else 1, 1 if c + 1 < chunks else rounds)
    for k in range(1, n):
        moments(1, k).start()

    pltpu.make_async_remote_copy(
        src_ref=ext.at[0:TERMS - 1, :, pl.ds(0, 2 * rim)], dst_ref=ext.at[0:TERMS - 1, :, pl.ds(0, 2 * rim)],
        send_sem=send_sem, recv_sem=msend, device_id={"slab": lax.rem(me + 1, n)},
        device_id_type=pl.DeviceIdType.MESH,
    ).wait_send()
    for c in range(chunks):
        for side in (near, far):
            held = LEAD if (TERMS - 1, c) == last and side is far else 0
            halo(TERMS - 1, c, side, 0, held, BAND).wait_send()
    for final in range(2):
        moments(final, 1, 0, n - 1).wait()


def finish(tb, mom, last_prev, last_cur, mom_hbm, row_sums, sem):
    n, terms, lanes_of, _ = mom.shape
    _, chunks, _, cc = tb.shape
    copies = []
    for c in range(chunks):
        for k, out in enumerate((last_cur, last_prev)):
            source = (terms - 1 + k) % 2
            copies.append(pltpu.make_async_copy(
                tb.at[source, c], out.at[:, pl.ds(c * cc, cc)], sem.at[2 * c + k]))
    for copy in copies:
        copy.start()
    for t in range(terms):
        whole = mom[0, t]
        for i in range(1, n):
            whole = whole + mom[i, t]
        for k in range(lanes_of):
            row_sums[t:t + 1, k * LANES:(k + 1) * LANES] = whole[k:k + 1, :]
    copies.append(pltpu.make_async_copy(row_sums, mom_hbm, sem.at[2 * chunks]))
    copies[-1].start()
    for copy in copies:
        copy.wait()


def local(hamiltonian_blocks, block_columns, probe, previous, current, orbital_weight):
    n = lax.axis_size("slab")
    rows, slots, w, _ = hamiltonian_blocks.shape
    height, cols = current.shape
    cc = min(CHUNK, cols)
    chunks = cols // cc
    vmem = pl.BlockSpec(memory_space=pltpu.VMEM)
    hbm = pl.BlockSpec(memory_space=pltpu.HBM)
    bf16, f32 = jnp.bfloat16, jnp.float32
    grant = 67043328 - 4 * (2 * height * cols + TERMS * n * cols) - (64 << 10)
    tb, mom = pl.pallas_call(
        functools.partial(kernel, n),
        out_shape=(
            pltpu.VMEM((2, chunks, height, cc), f32),
            pltpu.VMEM((n, TERMS, cols // LANES, LANES), f32),
        ),
        in_specs=[hbm] * 6,
        out_specs=(vmem, vmem),
        scratch_shapes=[
            pltpu.SMEM((rows, slots), jnp.int32),
            pltpu.VMEM((rows, w), f32),
            pltpu.VMEM((rows, slots, w, w), bf16),
            pltpu.VMEM((rows // GROUP, GROUP * w, (GROUP + 2 * BAND) * w), bf16),
            pltpu.VMEM((TERMS, chunks, height + 2 * BAND * w, cc), bf16),
            pltpu.VMEM((chunks, height, cc), f32),
            pltpu.VMEM((height, cols), bf16),
            pltpu.SemaphoreType.DMA((8 + 2 * chunks,)),
            pltpu.SemaphoreType.DMA,
            pltpu.SemaphoreType.DMA((2, chunks, 2, 2)),
            pltpu.SemaphoreType.DMA,
            pltpu.SemaphoreType.DMA((2,)),
            pltpu.SemaphoreType.REGULAR((max(1, (n // 2 - 1).bit_length()),)),
            pltpu.SemaphoreType.DMA,
            pltpu.SemaphoreType.REGULAR,
        ],
        compiler_params=pltpu.CompilerParams(
            collective_id=0, has_side_effects=True, vmem_limit_bytes=grant,
        ),
    )(block_columns, orbital_weight.reshape(rows, w), hamiltonian_blocks, probe, previous, current)
    return pl.pallas_call(
        finish,
        out_shape=(
            jax.ShapeDtypeStruct((height, cols), f32),
            jax.ShapeDtypeStruct((height, cols), f32),
            jax.ShapeDtypeStruct((TERMS, cols), f32),
        ),
        in_specs=[vmem, vmem],
        out_specs=(hbm, hbm, hbm),
        scratch_shapes=[
            pltpu.VMEM((TERMS, cols), f32),
            pltpu.SemaphoreType.DMA((2 * chunks + 1,)),
        ],
        compiler_params=pltpu.CompilerParams(vmem_limit_bytes=16 * 1024 * 1024),
    )(tb, mom)


def solution(mesh):
    return jax.shard_map(
        local,
        mesh=mesh,
        in_specs=(
            P("slab", None, None, None),
            P("slab", None),
            P("slab", "col"),
            P("slab", "col"),
            P("slab", "col"),
            P("slab"),
        ),
        out_specs=(P("slab", "col"), P("slab", "col"), P(None, "col")),
        check_vma=False,
    )
```

```python
import functools

import jax
import jax.numpy as jnp
from jax import lax
from jax.experimental import pallas as pl
from jax.experimental.pallas import tpu as pltpu
from jax.sharding import PartitionSpec as P

BAND = 5
TERMS = 3
LANES = 128
CHUNK = 256
GROUP = 2


def kernel(
    n, col_hbm, ow_hbm, h_hbm, probe_hbm, prev_hbm, cur_hbm,
    tb, mom, duo,
    col_ref, ow_ref, hv, hb, ext, wts, pv,
    in_sem, send_sem, recv_sem, msend, mrecv, known, gate_sem, turn,
):
    me = lax.axis_index("slab")
    rows, slots, w, _ = hv.shape
    chunks, height, cc = wts.shape
    total = n * rows
    rim = BAND * w
    gw = GROUP * w
    pairs = rows // GROUP
    edge = -(-BAND // GROUP)
    depth = gw + 2 * rim
    first = me * rows
    far = lax.rem(me, 2)
    near = 1 - far

    def columns(c):
        return pl.ds(c * cc, cc)

    inside = (BAND - GROUP) * w
    opening = (0, w // 8, 3 * w // 8, w, inside, rim)

    def parts(side):
        return ((0, inside), (inside, rim)) if side is far else ((0, rim),)

    def from_edge(side, a, b):
        return (1 - side) * a + side * (rim - b)

    def pieces(c, side):
        return tuple(zip(opening, opening[1:])) if c == 0 and side is far else ((0, rim),)

    def rim_in(c, side, k):
        a, b = pieces(c, side)[k]
        start = pl.multiple_of(side * (height - rim) + from_edge(side, a, b), w // 8)
        spot = k if c == 0 and side is far else len(opening) - 2 + 2 * c + (0 if side is far else 1)
        return pltpu.make_async_copy(
            cur_hbm.at[pl.ds(start, b - a), columns(c)],
            tb.at[1, c, pl.ds(start, b - a)],
            in_sem.at[6 + spot],
        )

    inner = height - 2 * rim
    inner_in = [
        pltpu.make_async_copy(
            cur_hbm.at[pl.ds(rim, inner), columns(c)], tb.at[1, c, pl.ds(rim, inner)],
            in_sem.at[0])
        for c in range(chunks)
    ]
    h_in = pltpu.make_async_copy(h_hbm, hv, in_sem.at[1])
    probe_in = pltpu.make_async_copy(probe_hbm, pv, in_sem.at[2])
    col_in = pltpu.make_async_copy(col_hbm, col_ref, in_sem.at[3])
    ow_in = pltpu.make_async_copy(ow_hbm, ow_ref, in_sem.at[4])
    prev_in = [
        pltpu.make_async_copy(prev_hbm.at[:, columns(c)], tb.at[0, c], in_sem.at[5])
        for c in range(chunks)
    ]
    barrier = pltpu.get_barrier_semaphore()

    def greet(semaphore, distance):
        for other in (n - distance, distance):
            pl.semaphore_signal(
                semaphore, inc=1, device_id={"slab": lax.rem(me + other, n)},
                device_id_type=pl.DeviceIdType.MESH,
            )

    greet(barrier, 1)
    for c in range(chunks):
        for side in (far, near):
            for k in range(len(pieces(c, side))):
                rim_in(c, side, k).start()

    def hops(chip):
        return lax.rem(chip, 2) + lax.rem(chip // 2, 2)

    chip = me // 2
    every = n // 2
    mine = hops(lax.rem(chip + every - 1 + 2 * far, every))
    other = hops(lax.rem(chip + every - 1 + 2 * near, every))
    last = (TERMS - 1, chunks - 1)

    def halo(t, c, side, part, a=None, b=None, gate=None):
        if a is None:
            a, b = parts(side)[part]
        size = b - a
        offset = from_edge(side, a, b)
        source = pl.multiple_of(rim + side * (height - rim) + offset, w // 8)
        target = pl.multiple_of((1 - side) * (rim + height) + offset, w // 8)
        return pltpu.make_async_remote_copy(
            src_ref=ext.at[t, c, pl.ds(source, size)],
            dst_ref=ext.at[t, c, pl.ds(target, size)],
            send_sem=send_sem if gate is None else gate,
            recv_sem=recv_sem.at[t % 2, c, 1 + part if side is far else 0],
            device_id={"slab": lax.rem(me + n - 1 + 2 * side, n)},
            device_id_type=pl.DeviceIdType.MESH,
        )

    def arrival(t, c, side, part):
        a, b = parts(side)[part]
        start = pl.multiple_of(side * (rim + height) + (1 - side) * (rim - b) + side * a, w // 8)
        landed = ext.at[t, c, pl.ds(start, b - a)]
        return pltpu.make_async_remote_copy(
            src_ref=landed, dst_ref=landed, send_sem=send_sem,
            recv_sem=recv_sem.at[t % 2, c, 1 + part if side is far else 0],
            device_id={"slab": lax.rem(me + n - 1 + 2 * side, n)},
            device_id_type=pl.DeviceIdType.MESH,
        )

    def cast(c, start, size):
        step = min(size, w)

        def body(i, carry):
            at = pl.multiple_of(start + i * step, w // 8)
            ext[0, c, pl.ds(pl.multiple_of(rim + at, w // 8), step)] = tb[1, c, pl.ds(at, step)].astype(jnp.bfloat16)
            return carry

        lax.fori_loop(0, size // step, body, 0)

    rounds = known.shape[0]
    for c in range(chunks):
        for side in (far, near):
            for k, (a, b) in enumerate(pieces(c, side)):
                rim_in(c, side, k).wait()
                cast(c, side * (height - rim) + from_edge(side, a, b), b - a)
                if c == 0 and side is far and k == 0:
                    pl.semaphore_wait(barrier, 2)
                for part, (low, high) in enumerate(parts(side)):
                    low, high = max(low, a), min(high, b)
                    if low < high:
                        halo(0, c, side, part, low, high).start()
            if c == 0 and side is far:
                for copy in inner_in:
                    copy.start()
                col_in.start()
                h_in.start()
                ow_in.start()
                probe_in.start()
                for copy in prev_in:
                    copy.start()
                greet(known.at[0], 1)
    inside_of = tb.at[1, :, pl.ds(rim, inner)]
    pltpu.make_async_copy(inside_of, inside_of, in_sem.at[0]).wait()
    for c in range(chunks):
        cast(c, rim, inner)

    col_in.wait()
    h_in.wait()
    zero = jnp.zeros((w, w), jnp.bfloat16)

    def build(p, carry):
        for half in range(GROUP):
            r = p * GROUP + half
            places = []
            for s in range(slots):
                x = col_ref[r, s] - (first + r) + BAND
                x = jnp.where(x < 0, x + total, x)
                places.append(jnp.where(x >= total, x - total, x))
            for d in range(GROUP + 2 * BAND):
                place = d - half
                if place < 0 or place > 2 * BAND:
                    block = zero
                else:
                    slot = jnp.int32(0)
                    hit = jnp.int32(0)
                    for s in range(slots):
                        same = places[s] == place
                        slot = jnp.where(same, s, slot)
                        hit = jnp.where(same, 1, hit)
                    block = jnp.where(hit == 1, hv[r, slot], zero)
                hb[p, half * w:(half + 1) * w, d * w:(d + 1) * w] = block
        return carry

    lax.fori_loop(0, pairs, build, 0)

    probe_in.wait()
    ow_in.wait()
    eye = lax.broadcasted_iota(jnp.int32, (w, w), 0) == lax.broadcasted_iota(jnp.int32, (w, w), 1)

    def weigh(r, carry):
        row = jnp.broadcast_to(ow_ref[pl.ds(r, 1), :], (w, w))
        column = jnp.sum(jnp.where(eye, row, 0.0), axis=1, keepdims=True) / (total * w)
        at = pl.multiple_of(r * w, w)
        for c in range(chunks):
            wts[c, pl.ds(at, w)] = column * pv[pl.ds(at, w), c * cc:(c + 1) * cc].astype(jnp.float32)
        return carry

    lax.fori_loop(0, rows, weigh, 0)
    pltpu.make_async_copy(tb.at[0], tb.at[0], in_sem.at[5]).wait()

    def tile(t, c, p, acc):
        at = pl.multiple_of(p * gw, gw)
        product = jnp.dot(hb[p], ext[t, c, pl.ds(at, depth)], preferred_element_type=jnp.float32)
        upcoming = 2.0 * product - tb[t % 2, c, pl.ds(at, gw)]
        tb[t % 2, c, pl.ds(at, gw)] = upcoming
        if t + 1 < TERMS:
            ext[t + 1, c, pl.ds(pl.multiple_of(rim + at, w), gw)] = upcoming.astype(jnp.bfloat16)
        y = wts[c, pl.ds(at, gw)] * upcoming
        return acc + jnp.sum(y.reshape(gw // 8, 8, cc), axis=0)

    late = rim - inside

    def split_tile(t, c, side, acc):
        p = side * (pairs - 1)
        at = pl.multiple_of(p * gw, gw)
        rows_of = pl.ds(at, gw)

        def twice(offset, size):
            offset = pl.multiple_of(offset, w)
            return 2.0 * jnp.dot(
                hb[p, :, pl.ds(offset, size)], ext[t, c, pl.ds(pl.multiple_of(at + offset, w), size)],
                preferred_element_type=jnp.float32)

        def weighed(value):
            return jnp.sum((wts[c, rows_of] * value).reshape(gw // 8, 8, cc), axis=0)

        begun = twice((1 - side) * late, depth - late) - tb[t % 2, c, rows_of]
        tb[t % 2, c, rows_of] = begun
        acc = acc + weighed(begun)
        arrival(t, c, side, 1).wait_recv()
        rest = twice(side * (depth - late), late)
        tb[t % 2, c, rows_of] = tb[t % 2, c, rows_of] + rest
        return acc + weighed(rest)

    def to(block, k, semaphore):
        return pltpu.make_async_remote_copy(
            src_ref=block, dst_ref=block, send_sem=msend, recv_sem=mrecv.at[semaphore],
            device_id={"slab": lax.rem(me + k, n)}, device_id_type=pl.DeviceIdType.MESH,
        )

    partner = n - 1 + 2 * near
    early = pl.ds(0, TERMS - 1)
    pair = to(mom.at[me, early], partner, 2)

    def spread(start, stop):
        for k in range(start, stop):
            pl.semaphore_wait(known.at[k], 2)
            if k + 1 < rounds:
                greet(known.at[k + 1], 2 ** (k + 1))

    for t in range(TERMS):
        for c in range(chunks):
            acc = jnp.zeros((8, cc), jnp.float32)
            acc = lax.fori_loop(edge, pairs - edge, lambda p, a: tile(t, c, p, a), acc)
            for side in (near, far):
                def rim_tile(i, a):
                    return tile(t, c, (1 - side) * (edge - 1 - i) + side * (pairs - edge + i), a)

                if (t, c) == last and side is far:
                    halo(t, c, side, 0, gate=gate_sem).wait_send()

                    @pl.when(mine > other)
                    def _():
                        pl.semaphore_signal(
                            turn, inc=1, device_id={"slab": lax.rem(me + n - 1 + 2 * near, n)},
                            device_id_type=pl.DeviceIdType.MESH)

                    @pl.when(mine < other)
                    def _():
                        pl.semaphore_wait(turn, 1)
                        halo(t, c, side, 1).start()

                arrival(t, c, side, 0).wait_recv()
                acc = lax.fori_loop(0, edge - 1, rim_tile, acc)
                if (t, c) == last and side is far:
                    for k in range(2, n, 2):
                        to(duo.at[chip], k, 0).start()
                if (t, c) == last and side is far:
                    acc = split_tile(t, c, side, acc)
                else:
                    if side is far:
                        arrival(t, c, side, 1).wait_recv()
                    acc = rim_tile(edge - 1, acc)
                if t + 1 < TERMS:
                    if (t + 1, c) == last and side is far:
                        halo(t + 1, c, side, 0, gate=gate_sem).start()
                        pl.when(mine >= other)(halo(t + 1, c, side, 1).start)
                    else:
                        for part in range(len(parts(side))):
                            halo(t + 1, c, side, part).start()
            total_row = jnp.sum(acc, axis=0, keepdims=True)
            for k in range(cc // LANES):
                mom[me, t, pl.ds(c * (cc // LANES) + k, 1), :] = total_row[:, k * LANES:(k + 1) * LANES]
            if t == TERMS - 1 and c == 0:
                pair.wait_recv()
                duo[chip] = mom[me, 0:TERMS - 1] + mom[lax.rem(me + partner, n), 0:TERMS - 1]
            if t == TERMS - 2 and c + 1 == chunks:
                pair.start()
            if t == 0:
                spread(0 if c == 0 else 1, 1 if c + 1 < chunks else rounds)
    for k in range(1, n):
        to(mom.at[me, TERMS - 1], k, 1).start()

    pltpu.make_async_remote_copy(
        src_ref=ext.at[0:TERMS - 1, :, pl.ds(0, 2 * rim)], dst_ref=ext.at[0:TERMS - 1, :, pl.ds(0, 2 * rim)],
        send_sem=send_sem, recv_sem=msend, device_id={"slab": lax.rem(me + 1, n)},
        device_id_type=pl.DeviceIdType.MESH,
    ).wait_send()
    for c in range(chunks):
        for side in (near, far):
            held = inside if (TERMS - 1, c) == last and side is far else 0
            halo(TERMS - 1, c, side, 0, held, rim).wait_send()
    pair.wait_send()
    to(duo.at[pl.ds(0, n // 2 - 1)], 1, 0).wait()
    to(mom.at[pl.ds(0, n - 1), TERMS - 1], 1, 1).wait()


def finish(tb, mom, duo, last_prev, last_cur, mom_hbm, row_sums, sem):
    n, terms, lanes_of, _ = mom.shape
    _, chunks, _, cc = tb.shape
    copies = []
    for c in range(chunks):
        for k, out in enumerate((last_cur, last_prev)):
            source = (terms - 1 + k) % 2
            copies.append(pltpu.make_async_copy(
                tb.at[source, c], out.at[:, pl.ds(c * cc, cc)], sem.at[2 * c + k]))
    for copy in copies:
        copy.start()
    for t in range(terms):
        kept, count = (mom, n) if t == terms - 1 else (duo, n // 2)
        whole = kept[0, t]
        for i in range(1, count):
            whole = whole + kept[i, t]
        for k in range(lanes_of):
            row_sums[t:t + 1, k * LANES:(k + 1) * LANES] = whole[k:k + 1, :]
    copies.append(pltpu.make_async_copy(row_sums, mom_hbm, sem.at[2 * chunks]))
    copies[-1].start()
    for copy in copies:
        copy.wait()


def local(hamiltonian_blocks, block_columns, probe, previous, current, orbital_weight):
    n = lax.axis_size("slab")
    rows, slots, w, _ = hamiltonian_blocks.shape
    height, cols = current.shape
    cc = min(CHUNK, cols)
    chunks = cols // cc
    vmem = pl.BlockSpec(memory_space=pltpu.VMEM)
    hbm = pl.BlockSpec(memory_space=pltpu.HBM)
    bf16, f32 = jnp.bfloat16, jnp.float32
    grant = 67043328 - 4 * (2 * height * cols + 2 * TERMS * n * cols) - (64 << 10)
    tb, mom, duo = pl.pallas_call(
        functools.partial(kernel, n),
        out_shape=(
            pltpu.VMEM((2, chunks, height, cc), f32),
            pltpu.VMEM((n, TERMS, cols // LANES, LANES), f32),
            pltpu.VMEM((n // 2, TERMS - 1, cols // LANES, LANES), f32),
        ),
        in_specs=[hbm] * 6,
        out_specs=(vmem, vmem, vmem),
        scratch_shapes=[
            pltpu.SMEM((rows, slots), jnp.int32),
            pltpu.VMEM((rows, w), f32),
            pltpu.VMEM((rows, slots, w, w), bf16),
            pltpu.VMEM((rows // GROUP, GROUP * w, (GROUP + 2 * BAND) * w), bf16),
            pltpu.VMEM((TERMS, chunks, height + 2 * BAND * w, cc), bf16),
            pltpu.VMEM((chunks, height, cc), f32),
            pltpu.VMEM((height, cols), bf16),
            pltpu.SemaphoreType.DMA((10 + 2 * chunks,)),
            pltpu.SemaphoreType.DMA,
            pltpu.SemaphoreType.DMA((2, chunks, 3)),
            pltpu.SemaphoreType.DMA,
            pltpu.SemaphoreType.DMA((3,)),
            pltpu.SemaphoreType.REGULAR((max(1, (n // 2 - 1).bit_length()),)),
            pltpu.SemaphoreType.DMA,
            pltpu.SemaphoreType.REGULAR,
        ],
        compiler_params=pltpu.CompilerParams(
            collective_id=0, has_side_effects=True, vmem_limit_bytes=grant,
        ),
    )(block_columns, orbital_weight.reshape(rows, w), hamiltonian_blocks, probe, previous, current)
    return pl.pallas_call(
        finish,
        out_shape=(
            jax.ShapeDtypeStruct((height, cols), f32),
            jax.ShapeDtypeStruct((height, cols), f32),
            jax.ShapeDtypeStruct((TERMS, cols), f32),
        ),
        in_specs=[vmem, vmem, vmem],
        out_specs=(hbm, hbm, hbm),
        scratch_shapes=[
            pltpu.VMEM((TERMS, cols), f32),
            pltpu.SemaphoreType.DMA((2 * chunks + 1,)),
        ],
        compiler_params=pltpu.CompilerParams(vmem_limit_bytes=16 * 1024 * 1024),
    )(tb, mom, duo)


def solution(mesh):
    return jax.shard_map(
        local,
        mesh=mesh,
        in_specs=(
            P("slab", None, None, None),
            P("slab", None),
            P("slab", "col"),
            P("slab", "col"),
            P("slab", "col"),
            P("slab"),
        ),
        out_specs=(P("slab", "col"), P("slab", "col"), P(None, "col")),
        check_vma=False,
    )
```
